32 devices in a mesh: batch: 4 (over z), row: 4 (over x, core), col: 2 (over y).
Axes of the slice: x: 2, y: 2, z: 4, core: 2. Of those that a mesh axis runs over, the one named last changes fastest.
Arguments:
- features: bfloat16 [4, 64, 256, 320], P('batch', 'row', 'col'), may hold values from -6 to 6
- first_kernel: bfloat16 [3, 3, 320, 320], replicated, may hold values from -0.109375 to 0.109375
- second_kernel: bfloat16 [3, 3, 320, 320], replicated, may hold values from -0.109375 to 0.109375
- first_gain: float32 [320], replicated, may hold values from 0.5 to 1.5
- first_shift: float32 [320], replicated, may hold values from -3 to 3
- second_gain: float32 [320], replicated, may hold values from 0.5 to 1.5
- second_shift: float32 [320], replicated, may hold values from -3 to 3
- upstream: bfloat16 [4, 64, 256, 320], P('batch', 'row', 'col'), may hold values from -6 to 6
Outputs:
- input_grad: bfloat16 [4, 64, 256, 320], P('batch', 'row', 'col')
- first_kernel_grad: float32 [3, 3, 320, 320], replicated
- second_kernel_grad: float32 [3, 3, 320, 320], replicated
- norm_param_grads: float32 [4, 320], replicated
The draws below stay inside these ranges and needn't reach their ends.
All inputs are finite; a program needn't handle non-finite values.
Results may differ from the reference program's by a relative error of at most 0.002.
The reference program's roundings to bfloat16 on the way (of `act_one`, `hidden`, `act_two` and `grad_hidden`) count: a program that leaves them out, or rounds other values in their place, can miss the bound.
Values may be sent and summed in bfloat16 or wider, within the bound.
No kernel may reach another device: no remote copies, remote signals or barrier semaphores. Data moves between devices by JAX's collectives and lax.ppermute only.
A program may use at most 128 MiB of HBM per device.

```python
import jax
import jax.numpy as jnp
from jax import lax

C = 320
GROUPS = 32
KS = 3
B = 4
H = 64
W = 256


def shard_levels(own_key, shape, shards, least, largest):
    level = 1.0
    for position, shards_of in shards:
        heights = jax.random.uniform(jax.random.fold_in(jax.random.fold_in(own_key, 6), position), (shards_of,), jnp.float32, least / len(shards), largest / len(shards))
        level = level * jnp.repeat(jnp.exp(heights), shape[position] // shards_of).reshape((-1,) + (1,) * (len(shape) - 1 - position))
    return level


def scatter_about(key, extent, width, limit, cuts=(), held_as=jnp.bfloat16):
    drawn = jax.random.normal(key, extent, jnp.float32) * width
    if len(cuts) > 0:
        drawn = shard_levels(key, extent, cuts, -0.22, 0.18) * drawn
    return jnp.clip(drawn, min=-limit, max=limit).astype(held_as)


def setup_inputs(seed: int = 0) -> dict:
    arg_keys = jax.random.split(jax.random.key(seed), 9)
    return {
        "features": scatter_about(arg_keys[0], (B, H, W, C), 1.0, 6.0, ((0, 4), (1, 4), (2, 2))),
        "first_kernel": scatter_about(arg_keys[1], (KS, KS, C, C), (KS * KS * C) ** -0.5, 0.109375),
        "second_kernel": scatter_about(arg_keys[2], (KS, KS, C, C), (KS * KS * C) ** -0.5, 0.109375),
        "first_gain": jnp.clip(1.0 + 0.1 * jax.random.normal(arg_keys[3], (C,), jnp.float32), 0.5, 1.5),
        "first_shift": scatter_about(arg_keys[4], (C,), 0.5, 3.0, (), jnp.float32),
        "second_gain": jnp.clip(1.0 + 0.1 * jax.random.normal(arg_keys[5], (C,), jnp.float32), 0.5, 1.5),
        "second_shift": scatter_about(arg_keys[6], (C,), 0.5, 3.0, (), jnp.float32),
        "upstream": scatter_about(arg_keys[7], (B, H, W, C), 1.0, 6.0, ((0, 4), (1, 4), (2, 2))),
    }


EPS = 1e-05
HIGH = lax.Precision.HIGHEST

def conv_same(values, kernel):
    return lax.conv_general_dilated(values.astype(jnp.float32), kernel.astype(jnp.float32), (1, 1), ((1, 1), (1, 1)), dimension_numbers=('NHWC', 'HWIO', 'NHWC'), precision=HIGH)

def flipped(kernel):
    return jnp.transpose(jnp.flip(kernel, (0, 1)), (0, 1, 3, 2))

def kernel_grad(values, gradient):
    padded = jnp.pad(values.astype(jnp.float32), ((0, 0), (1, 1), (1, 1), (0, 0)))
    height, breadth, chans = (gradient.shape[1], gradient.shape[2], gradient.shape[3])
    flat_grad = gradient.astype(jnp.float32).reshape(-1, chans)
    pieces = []
    for offset in range(9):
        across, along = (offset // 3, offset % 3)
        window = padded[:, across:across + height, along:along + breadth, :].reshape(-1, values.shape[3])
        pieces.append(lax.dot_general(window, flat_grad, (((0,), (0,)), ((), ())), precision=HIGH))
    return jnp.stack(pieces).reshape(3, 3, values.shape[3], chans)

def moments(values):
    bsize, chans = (values.shape[0], values.shape[3])
    grouped = values.reshape(bsize, -1, GROUPS, chans // GROUPS)
    center = lax.optimization_barrier(jnp.mean(grouped, axis=(1, 3), keepdims=True))
    shifted = grouped - center
    spread = lax.optimization_barrier(jnp.mean(shifted * shifted, axis=(1, 3), keepdims=True))
    rstd = lax.rsqrt(spread + EPS)
    return ((shifted * rstd).reshape(values.shape), rstd)

def silu_grad(grad_act, pre):
    sigma = jax.nn.sigmoid(pre)
    return grad_act * sigma * (1.0 + pre * (1.0 - sigma))

def norm_back(grad_pre, normal, rstd, gain):
    bsize, chans = (grad_pre.shape[0], grad_pre.shape[3])
    count = grad_pre.shape[1] * grad_pre.shape[2] * (chans // GROUPS)
    shift_sum = lax.optimization_barrier(jnp.sum(grad_pre, axis=(1, 2)))
    gain_sum = lax.optimization_barrier(jnp.sum(grad_pre * normal, axis=(1, 2)))
    mean_one = lax.optimization_barrier(jnp.sum((shift_sum * gain).reshape(bsize, GROUPS, -1), axis=2)) / count
    mean_two = lax.optimization_barrier(jnp.sum((gain_sum * gain).reshape(bsize, GROUPS, -1), axis=2)) / count
    scaled = (grad_pre * gain).reshape(bsize, -1, GROUPS, chans // GROUPS)
    normal_grouped = normal.reshape(scaled.shape)
    grad_in = rstd * (scaled - mean_one[:, None, :, None] - normal_grouped * mean_two[:, None, :, None])
    return (grad_in.reshape(grad_pre.shape), lax.optimization_barrier(jnp.sum(gain_sum, axis=0)), lax.optimization_barrier(jnp.sum(shift_sum, axis=0)))

def reference(features, first_kernel, second_kernel, first_gain, first_shift, second_gain, second_shift, upstream):
    normal_one, rstd_one = moments(features.astype(jnp.float32))
    pre_one = normal_one * first_gain + first_shift
    act_one = jax.nn.silu(pre_one).astype(jnp.bfloat16)
    hidden = conv_same(act_one, first_kernel).astype(jnp.bfloat16)
    normal_two, rstd_two = moments(hidden.astype(jnp.float32))
    pre_two = normal_two * second_gain + second_shift
    act_two = jax.nn.silu(pre_two).astype(jnp.bfloat16)
    second_kernel_grad = kernel_grad(act_two, upstream)
    grad_pre_two = silu_grad(conv_same(upstream, flipped(second_kernel)), pre_two)
    grad_hidden, gain_two, shift_two = norm_back(grad_pre_two, normal_two, rstd_two, second_gain)
    grad_hidden = grad_hidden.astype(jnp.bfloat16)
    first_kernel_grad = kernel_grad(act_one, grad_hidden)
    grad_pre_one = silu_grad(conv_same(grad_hidden, flipped(first_kernel)), pre_one)
    grad_input, gain_one, shift_one = norm_back(grad_pre_one, normal_one, rstd_one, first_gain)
    input_grad = (upstream.astype(jnp.float32) + grad_input).astype(jnp.bfloat16)
    norm_param_grads = jnp.stack([gain_one, shift_one, gain_two, shift_two])
    return (input_grad, first_kernel_grad, second_kernel_grad, norm_param_grads)
```

```python
import functools

import jax
import jax.numpy as jnp
from jax import lax
from jax.experimental import pallas as pl
from jax.experimental.pallas import tpu as pltpu
from jax.sharding import PartitionSpec as P

GROUPS = 32
EPS = 1e-05
F32 = jnp.float32
BF16 = jnp.bfloat16
CHUNK = 4
VMEM = pl.BlockSpec(memory_space=pltpu.VMEM)
SMEM = pl.BlockSpec(memory_space=pltpu.SMEM)
AXES = ("batch", "row", "col")


def call(body, out_shape, n_in, scratch=(), flags=True):
    return pl.pallas_call(
        body,
        out_shape=out_shape,
        in_specs=([SMEM] if flags else []) + [VMEM] * n_in,
        out_specs=jax.tree.map(lambda _: VMEM, out_shape),
        scratch_shapes=list(scratch),
    )


def shape(dims, dtype):
    return jax.ShapeDtypeStruct(dims, dtype)


def group_total(rows):
    chans = rows.shape[1]
    width = chans // GROUPS
    left = lax.broadcasted_iota(jnp.int32, (chans, chans), 0).astype(F32)
    right = lax.broadcasted_iota(jnp.int32, (chans, chans), 1).astype(F32)
    same = jnp.floor((left + 0.5) / width) == jnp.floor((right + 0.5) / width)
    return jnp.dot(
        rows,
        same.astype(F32),
        precision=lax.Precision.HIGHEST,
        preferred_element_type=F32,
    )


def mean_rstd(stats, count):
    total = group_total(stats)
    mean = total[0:1] / count
    spread = total[1:2] / count - mean * mean
    return mean, lax.rsqrt(spread + EPS)


def silu(pre):
    return pre / (1.0 + jnp.exp(-pre))


def silu_slope(pre):
    sigma = 1.0 / (1.0 + jnp.exp(-pre))
    return sigma * (1.0 + pre * (1.0 - sigma))


def pair_rows(first, second):
    rows = lax.broadcasted_iota(jnp.int32, (8, first.shape[1]), 0)
    return jnp.where(rows == 0, first, jnp.where(rows == 1, second, 0.0))


def fold(block):
    return jnp.sum(block.reshape(block.shape[0] // 8, 8, block.shape[1]), axis=0)


def build_taps(flags, core, top, bottom, left, right, taps, line, sides, act):
    high, wide, chans = core.shape
    has_top, has_bottom = flags[0] > 0, flags[1] > 0
    has_left, has_right = flags[2] > 0, flags[3] > 0
    index = lax.broadcasted_iota(jnp.int32, (sides.shape[1], 1), 0)
    inside = ((index > 0) | has_top) & ((index < high + 1) | has_bottom) & (index < high + 2)
    sides[0] = jnp.where(inside & has_left, act(left[...].astype(F32)), 0.0)
    sides[1] = jnp.where(inside & has_right, act(right[...].astype(F32)), 0.0)

    def put(position, cells):
        line[7:8, :] = sides[0, pl.ds(position, 1), :]
        line[8 : 8 + wide, :] = cells
        line[8 + wide : 9 + wide, :] = sides[1, pl.ds(position, 1), :]
        for tap in range(3):
            taps[position, :, tap * chans : (tap + 1) * chans] = line[
                7 + tap : 7 + tap + wide, :
            ].astype(BF16)

    put(0, jnp.where(has_top, act(top[...].astype(F32)), 0.0))
    put(high + 1, jnp.where(has_bottom, act(bottom[...].astype(F32)), 0.0))

    def step(row, carry):
        put(row + 1, act(core[row].astype(F32)))
        return carry

    lax.fori_loop(0, high, step, 0)


def flip_weights(kernel, turned):
    chans = turned.shape[1]
    for across in range(3):
        for along in range(3):
            tap = 3 * (2 - across) + 2 - along
            turned[across, :, along * chans : (along + 1) * chans] = kernel[
                tap * chans : (tap + 1) * chans, :
            ]


def conv_rows(taps, weight, first, rows, turned):
    wide, depth = taps.shape[1], taps.shape[2]
    total = None
    for across in range(3):
        cells = taps[pl.ds(first + across, rows)].reshape(rows * wide, depth)
        dims = (((1,), (1 if turned else 0,)), ((), ()))
        part = lax.dot_general(cells, weight(across), dims, preferred_element_type=F32)
        total = part if total is None else total + part
    return total


def look_kernel(flags, core, upstream, stats, tops, bottoms, lefts, rights, edge):
    high, wide, chans = core.shape

    def step(row, carry):
        cells = core[row].astype(F32)
        return carry[0] + fold(cells), carry[1] + fold(cells * cells)

    zero = jnp.zeros((8, chans), F32)
    total, square = lax.fori_loop(0, high, step, (zero, zero))
    stats[...] = pair_rows(
        jnp.sum(total, axis=0, keepdims=True), jnp.sum(square, axis=0, keepdims=True)
    )
    for which, array in enumerate((core, upstream)):
        tops[which] = array[0]
        bottoms[which] = array[high - 1]
        for target, at in ((lefts, 0), (rights, wide - 8)):
            inner = 0 if at == 0 else 7
            for row in range(high):
                strip = array[row, at : at + 8, :].astype(F32)
                edge[row : row + 1, :] = strip[inner : inner + 1, :]
            target[which] = edge[...].astype(BF16)


def sides_kernel(edges, above, below, out, line, *, at):
    count, high, chans = edges.shape
    out_high = out.shape[1]
    inner = 0 if at == 0 else 7
    for which in range(count):
        line[...] = jnp.zeros_like(line)
        line[0:1, :] = above[which, at : at + 8, :].astype(F32)[inner : inner + 1, :]
        line[1 : 1 + high, :] = edges[which].astype(F32)
        line[1 + high : 2 + high, :] = below[which, at : at + 8, :].astype(F32)[
            inner : inner + 1, :
        ]
        out[which] = line[...].astype(BF16)


def identity(cells):
    return cells


def hidden_kernel(
    flags, core, top, bottom, left, right, kernel, stats, gain, shift,
    hidden, sums, taps, line, sides, *, count,
):
    high, wide, chans = core.shape
    mean, rstd = mean_rstd(stats[...], count)
    scale = rstd * gain[...]
    offset = shift[...] - mean * scale
    build_taps(
        flags, core, top, bottom, left, right, taps, line, sides,
        lambda cells: silu(cells * scale + offset),
    )
    depth = taps.shape[2]

    def step(index, carry):
        block = conv_rows(
            taps,
            lambda across: kernel[across * depth : (across + 1) * depth, :],
            index * CHUNK, CHUNK, False,
        ).astype(BF16)
        hidden[pl.ds(index * CHUNK * wide, CHUNK * wide), :] = block
        wideb = block.astype(F32)
        return carry[0] + fold(wideb), carry[1] + fold(wideb * wideb)

    zero = jnp.zeros((8, chans), F32)
    total, square = lax.fori_loop(0, high // CHUNK, step, (zero, zero))
    sums[...] = pair_rows(
        jnp.sum(total, axis=0, keepdims=True), jnp.sum(square, axis=0, keepdims=True)
    )


def back_conv_kernel(
    flags, core, top, bottom, left, right, kernel, out, taps, line, sides, turned
):
    high, wide, chans = core.shape
    build_taps(flags, core, top, bottom, left, right, taps, line, sides, identity)
    flip_weights(kernel, turned)

    def step(index, carry):
        out[pl.ds(index * CHUNK * wide, CHUNK * wide), :] = conv_rows(
            taps, lambda across: turned[across], index * CHUNK, CHUNK, True
        )
        return carry

    lax.fori_loop(0, high // CHUNK, step, 0)


def slope_kernel(grad, hidden, stats, gain, shift, out, sums, *, count):
    mean, rstd = mean_rstd(stats[...], count)
    chans = grad.shape[1]
    size = 256

    def step(index, carry):
        window = pl.ds(index * size, size)
        normal = (hidden[window, :].astype(F32) - mean) * rstd
        block = grad[window, :] * silu_slope(normal * gain[...] + shift[...])
        out[window, :] = block
        return carry[0] + fold(block), carry[1] + fold(block * normal)

    zero = jnp.zeros((8, chans), F32)
    total, product = lax.fori_loop(0, grad.shape[0] // size, step, (zero, zero))
    sums[...] = pair_rows(
        jnp.sum(total, axis=0, keepdims=True), jnp.sum(product, axis=0, keepdims=True)
    )


def norm_back_terms(stats, sums, gain, count):
    mean, rstd = mean_rstd(stats[...], count)
    means = group_total(sums[...] * gain[...]) / count
    return mean, rstd, means[0:1], means[1:2]


def grad_hidden_kernel(
    grad_pre, hidden, stats, sums, gain, out, tops, bottoms, lefts, rights, edge, *, count
):
    mean, rstd, mean_one, mean_two = norm_back_terms(stats, sums, gain, count)
    high, wide, chans = out.shape

    def step(row, carry):
        window = pl.ds(row * wide, wide)
        normal = (hidden[window, :].astype(F32) - mean) * rstd
        block = rstd * (grad_pre[window, :] * gain[...] - mean_one - normal * mean_two)
        out[row] = block.astype(BF16)
        return carry

    lax.fori_loop(0, high, step, 0)
    tops[0] = out[0]
    bottoms[0] = out[high - 1]
    for target, at in ((lefts, 0), (rights, wide - 8)):
        inner = 0 if at == 0 else 7
        for row in range(high):
            strip = out[row, at : at + 8, :].astype(F32)
            edge[row : row + 1, :] = strip[inner : inner + 1, :]
        target[0] = edge[...].astype(BF16)


def input_grad_kernel(grad_pre, core, upstream, stats, sums, gain, out, *, count):
    mean, rstd, mean_one, mean_two = norm_back_terms(stats, sums, gain, count)
    high, wide, chans = out.shape

    def step(row, carry):
        window = pl.ds(row * wide, wide)
        normal = (core[row].astype(F32) - mean) * rstd
        block = rstd * (grad_pre[window, :] * gain[...] - mean_one - normal * mean_two)
        out[row] = (upstream[row].astype(F32) + block).astype(BF16)
        return carry

    lax.fori_loop(0, high, step, 0)


def scatter_blocks(places, natural, out, size):
    for block in range(out.shape[0] // size):
        at = pl.multiple_of(places[block] * size, 8)
        out[block * size : (block + 1) * size, :] = natural[pl.ds(at, size), :]


def second_grad_kernel(
    flags, places, core, top, bottom, left, right, hidden, stats, gain, shift,
    out, taps, line, sides, turned, natural, *, count, size,
):
    high, wide, chans = core.shape
    build_taps(flags, core, top, bottom, left, right, taps, line, sides, identity)
    mean, rstd = mean_rstd(stats[...], count)
    scale = rstd * gain[...]
    offset = shift[...] - mean * scale
    depth = taps.shape[2]
    for part in range(high * wide // 256):
        window = slice(part * 256, (part + 1) * 256)
        act = silu(hidden[window, :].astype(F32) * scale + offset)
        turned[:, window] = act.astype(BF16).T
    for across in range(3):
        cells = taps[2 - across : 2 - across + high].reshape(high * wide, depth)
        block = jnp.dot(turned[...], cells, preferred_element_type=F32)
        for along in range(3):
            lanes = slice((2 - along) * chans, (3 - along) * chans)
            first = (3 * across + along) * chans
            natural[first : first + chans, :] = block[:, lanes]
    natural[9 * chans :, :] = jnp.zeros_like(natural[9 * chans :, :])
    scatter_blocks(places, natural, out, size)


def first_grad_kernel(
    flags, places, core, top, bottom, left, right, grad_hidden, stats, gain, shift,
    out, taps, line, sides, turned, natural, *, count, size,
):
    high, wide, chans = core.shape
    mean, rstd = mean_rstd(stats[...], count)
    scale = rstd * gain[...]
    offset = shift[...] - mean * scale
    build_taps(
        flags, core, top, bottom, left, right, taps, line, sides,
        lambda cells: silu(cells * scale + offset),
    )
    depth = taps.shape[2]
    for part in range(high * wide // 256):
        rows = 256 // wide
        cells = grad_hidden[part * rows : (part + 1) * rows].reshape(256, chans)
        turned[:, part * 256 : (part + 1) * 256] = cells.T
    for across in range(3):
        cells = taps[across : across + high].reshape(high * wide, depth)
        block = jnp.dot(turned[...], cells, preferred_element_type=F32)
        natural[across * depth : (across + 1) * depth, :] = block.T
    natural[9 * chans :, :] = jnp.zeros_like(natural[9 * chans :, :])
    scatter_blocks(places, natural, out, size)


def spread_kernel(places, mine, out, natural, *, size):
    for block in range(mine.shape[0] // size):
        at = pl.multiple_of(places[block] * size, 8)
        natural[pl.ds(at, size), :] = mine[block * size : (block + 1) * size, :].astype(F32)
    out[...] = natural[: out.shape[0], :]


def swap(value, axis, mask):
    return lax.ppermute(value, axis, [(i, i ^ mask) for i in range(lax.axis_size(axis))])


def bits_of(axis):
    count = lax.axis_size(axis)
    assert count & (count - 1) == 0
    return [(axis, 1 << bit) for bit in range(count.bit_length() - 1)]


def add_up(value, axes):
    for axis in axes:
        for name, mask in bits_of(axis):
            value = value + swap(value, name, mask)
    return value


def shifted(value, axis, step):
    count = lax.axis_size(axis)
    pairs = [(i, i + step) for i in range(count) if 0 <= i + step < count]
    return lax.ppermute(value, axis, pairs)


def borders(tops, bottoms, lefts, rights):
    count, wide, chans = tops.shape
    high = lefts.shape[1]
    above = shifted(bottoms, "row", 1)
    below = shifted(tops, "row", -1)

    def column(edges, at):
        return call(
            functools.partial(sides_kernel, at=at),
            shape((count, high + 8, chans), BF16), 3,
            [pltpu.VMEM((high + 8, chans), F32)], flags=False,
        )(edges, above, below)

    from_left = shifted(column(rights, wide - 8), "col", 1)
    from_right = shifted(column(lefts, 0), "col", -1)
    return above, below, from_left, from_right


def plan():
    row, col, batch = bits_of("row"), bits_of("col"), bits_of("batch")
    return row[:1], row[1:] + col, batch


def exchange_orders():
    first, middle, last = plan()
    return (first + middle + last, first + middle[::-1] + last)


def places_of(blocks):
    half = blocks // 2
    levels = len(exchange_orders()[0])
    head = len(plan()[0])
    found = []
    for order in exchange_orders():
        own = 0
        for level, (axis, mask) in enumerate(order):
            bit = (lax.axis_index(axis) & mask) // mask
            weight = half >> (level + 1)
            if level < head:
                weight *= 2
            own = own + bit * weight
        found.append(own)
    outer = blocks >> head
    index = jnp.arange(blocks, dtype=jnp.int32)
    chunk = (index % outer) // (outer // 2)
    return index ^ jnp.where(chunk == 0, found[0], found[1])


def give_away(whole):
    first, middle, last = plan()
    for axis, mask in first:
        half = whole.shape[0] // 2
        whole = whole[:half] + swap(whole[half:], axis, mask)
    half = whole.shape[0] // 2
    chunks = [whole[:half], whole[half:]]
    for pair in zip(middle, middle[::-1], strict=True):
        chunks = [
            chunk[: chunk.shape[0] // 2] + swap(chunk[chunk.shape[0] // 2 :], axis, mask)
            for chunk, (axis, mask) in zip(chunks, pair, strict=True)
        ]
    both = jnp.stack(chunks)
    for axis, mask in last:
        half = both.shape[1] // 2
        both = both[:, :half] + swap(both[:, half:], axis, mask)
    return both


def collect(both):
    first, middle, last = plan()
    for axis, mask in last[::-1]:
        both = jnp.concatenate([both, swap(both, axis, mask)], axis=1)
    chunks = [both[0], both[1]]
    for pair in list(zip(middle, middle[::-1], strict=True))[::-1]:
        chunks = [
            jnp.concatenate([chunk, swap(chunk, axis, mask)])
            for chunk, (axis, mask) in zip(chunks, pair, strict=True)
        ]
    whole = jnp.concatenate(chunks)
    for axis, mask in first[::-1]:
        whole = jnp.concatenate([whole, swap(whole, axis, mask)])
    return whole


def per_device(
    features, first_kernel, second_kernel, first_gain, first_shift,
    second_gain, second_shift, upstream,
):
    high, wide, chans = features.shape[1:]
    rows, cols = lax.axis_size("row"), lax.axis_size("col")
    devices = rows * cols * lax.axis_size("batch")
    count = float(high * rows * wide * cols * (chans // GROUPS))
    cells = features[0]
    upper = upstream[0]
    weights = [k.reshape(9 * chans, chans) for k in (first_kernel, second_kernel)]
    gains = [g.reshape(1, chans) for g in (first_gain, second_gain)]
    shifts = [s.reshape(1, chans) for s in (first_shift, second_shift)]
    row, col = lax.axis_index("row"), lax.axis_index("col")
    flags = jnp.stack([row > 0, row < rows - 1, col > 0, col < cols - 1]).astype(jnp.int32)
    unit = 2 * devices * 16
    padded = -(-9 * chans // unit) * unit
    blocks = 2 * devices
    size = padded // blocks
    places = places_of(blocks)

    image = shape((high, wide, chans), BF16)
    flat = high * wide
    small = shape((8, chans), F32)
    rows_of = lambda n: shape((n, wide, chans), BF16)
    cols_of = lambda n: shape((n, high, chans), BF16)
    edge = pltpu.VMEM((high, chans), F32)
    tap_scratch = [
        pltpu.VMEM((high + 2, wide, 3 * chans), BF16),
        pltpu.VMEM((wide + 16, chans), F32),
        pltpu.VMEM((2, high + 8, chans), F32),
    ]

    stats_one, tops, bottoms, lefts, rights = call(
        look_kernel, (small, rows_of(2), rows_of(2), cols_of(2), cols_of(2)), 2, [edge]
    )(flags, cells, upper)
    above, below, from_left, from_right = borders(tops, bottoms, lefts, rights)
    halo_one = (above[0], below[0], from_left[0], from_right[0])
    halo_up = (above[1], below[1], from_left[1], from_right[1])
    stats_one = add_up(stats_one, ("row", "col"))

    hidden, stats_two = call(
        functools.partial(hidden_kernel, count=count),
        (shape((flat, chans), BF16), small), 9, tap_scratch,
    )(flags, cells, *halo_one, weights[0], stats_one, gains[0], shifts[0])
    stats_two = add_up(stats_two, ("row", "col"))

    back_conv = call(
        back_conv_kernel, shape((flat, chans), F32), 6,
        tap_scratch + [pltpu.VMEM((3, chans, 3 * chans), BF16)],
    )
    grad_act_two = back_conv(flags, upper, *halo_up, weights[1])

    slope = call(
        functools.partial(slope_kernel, count=count),
        (shape((flat, chans), F32), small), 5, flags=False,
    )
    grad_pre_two, local_two = slope(grad_act_two, hidden, stats_two, gains[1], shifts[1])
    sums_two = add_up(local_two, ("row", "col"))

    def kernel_grad_call(body):
        return pl.pallas_call(
            functools.partial(body, count=count, size=size),
            out_shape=shape((padded, chans), F32),
            in_specs=[SMEM, SMEM] + [VMEM] * 9,
            out_specs=VMEM,
            scratch_shapes=tap_scratch
            + [pltpu.VMEM((chans, flat), BF16), pltpu.VMEM((padded, chans), F32)],
        )

    second_local = kernel_grad_call(second_grad_kernel)(
        flags, places, upper, *halo_up, hidden, stats_two, gains[1], shifts[1]
    )
    second_part = give_away(second_local)

    grad_hidden, tops, bottoms, lefts, rights = call(
        functools.partial(grad_hidden_kernel, count=count),
        (image, rows_of(1), rows_of(1), cols_of(1), cols_of(1)), 5, [edge], flags=False,
    )(grad_pre_two, hidden, stats_two, sums_two, gains[1])
    halo_grad = [part[0] for part in borders(tops, bottoms, lefts, rights)]

    first_local = kernel_grad_call(first_grad_kernel)(
        flags, places, cells, *halo_one, grad_hidden, stats_one, gains[0], shifts[0]
    )
    first_part = give_away(first_local)

    grad_act_one = back_conv(flags, grad_hidden, *halo_grad, weights[0])
    grad_pre_one, local_one = slope(
        grad_act_one, cells.reshape(flat, chans), stats_one, gains[0], shifts[0]
    )
    sums_one = add_up(local_one, ("row", "col"))
    input_grad = call(
        functools.partial(input_grad_kernel, count=count), image, 6, flags=False
    )(grad_pre_one, cells, upper, stats_one, sums_one, gains[0])

    param = jnp.stack([sums_one[1], sums_one[0], sums_two[1], sums_two[0]])
    param = add_up(param, ("batch",))

    spread = pl.pallas_call(
        functools.partial(spread_kernel, size=size),
        out_shape=shape((9 * chans, chans), F32),
        in_specs=[SMEM, VMEM],
        out_specs=VMEM,
        scratch_shapes=[pltpu.VMEM((padded, chans), F32)],
    )
    grads = [
        spread(places, collect(part.astype(BF16))).reshape(3, 3, chans, chans)
        for part in (first_part, second_part)
    ]
    return (input_grad[None], grads[0], grads[1], param)


def solution(mesh):
    tiled = P("batch", "row", "col", None)
    return jax.shard_map(
        per_device,
        mesh=mesh,
        in_specs=(tiled, P(), P(), P(), P(), P(), P(), tiled),
        out_specs=(tiled, P(), P(), P()),
        check_vma=False,
    )
```

```python
import functools

import jax
import jax.numpy as jnp
from jax import lax
from jax.experimental import pallas as pl
from jax.experimental.pallas import tpu as pltpu
from jax.sharding import PartitionSpec as P

GROUPS = 32
EPS = 1e-05
F32 = jnp.float32
BF16 = jnp.bfloat16
CHUNK = 4
LANES = 128
LIMIT = 24 * 2**20
VMEM = pl.BlockSpec(memory_space=pltpu.VMEM)
SMEM = pl.BlockSpec(memory_space=pltpu.SMEM)


def call(body, out_shape, n_in, scratch=(), smem=0):
    return pl.pallas_call(
        body,
        out_shape=out_shape,
        in_specs=[SMEM] * smem + [VMEM] * n_in,
        out_specs=jax.tree.map(lambda _: VMEM, out_shape),
        scratch_shapes=list(scratch),
        compiler_params=pltpu.CompilerParams(vmem_limit_bytes=LIMIT),
    )


def shape(dims, dtype):
    return jax.ShapeDtypeStruct(dims, dtype)


def group_total(rows):
    chans = rows.shape[1]
    width = chans // GROUPS
    left = lax.broadcasted_iota(jnp.int32, (chans, chans), 0).astype(F32)
    right = lax.broadcasted_iota(jnp.int32, (chans, chans), 1).astype(F32)
    same = jnp.floor((left + 0.5) / width) == jnp.floor((right + 0.5) / width)
    return jnp.dot(
        rows,
        same.astype(F32),
        precision=lax.Precision.HIGHEST,
        preferred_element_type=F32,
    )


def mean_rstd(stats_a, stats_b, count):
    total = group_total(stats_a[...] + stats_b[...])
    mean = total[0:1] / count
    spread = total[1:2] / count - mean * mean
    return mean, lax.rsqrt(spread + EPS)


def silu(pre):
    return pre / (1.0 + jnp.exp(-pre))


def silu_slope(pre):
    sigma = 1.0 / (1.0 + jnp.exp(-pre))
    return sigma * (1.0 + pre * (1.0 - sigma))


def pair_rows(first, second):
    rows = lax.broadcasted_iota(jnp.int32, (8, first.shape[1]), 0)
    first = jnp.sum(first, axis=0, keepdims=True)
    second = jnp.sum(second, axis=0, keepdims=True)
    return jnp.where(rows == 0, first, jnp.where(rows == 1, second, 0.0))


def fold(block):
    return jnp.sum(block.reshape(block.shape[0] // 8, 8, block.shape[1]), axis=0)


def build_taps(flags, core, halo, which, taps, line, sides, act):
    high, wide, chans = core.shape
    top, bottom, left, right = (part.at[which] for part in halo)
    has_top, has_bottom = flags[0] > 0, flags[1] > 0
    has_left, has_right = flags[2] > 0, flags[3] > 0
    index = lax.broadcasted_iota(jnp.int32, (sides.shape[1], 1), 0)
    inside = ((index > 0) | has_top) & ((index < high + 1) | has_bottom) & (index < high + 2)
    sides[0] = jnp.where(inside & has_left, act(left[...].astype(F32)), 0.0)
    sides[1] = jnp.where(inside & has_right, act(right[...].astype(F32)), 0.0)

    def put(position, cells):
        line[7:8, :] = sides[0, pl.ds(position, 1), :]
        line[8 : 8 + wide, :] = cells
        line[8 + wide : 9 + wide, :] = sides[1, pl.ds(position, 1), :]
        for tap in range(3):
            taps[position, :, tap * chans : (tap + 1) * chans] = line[
                7 + tap : 7 + tap + wide, :
            ].astype(BF16)

    put(0, jnp.where(has_top, act(top[...].astype(F32)), 0.0))
    put(high + 1, jnp.where(has_bottom, act(bottom[...].astype(F32)), 0.0))

    def step(row, carry):
        put(row + 1, act(core[row].astype(F32)))
        return carry

    lax.fori_loop(0, high, step, 0)


def flip_weights(kernel, turned):
    chans = turned.shape[1]
    for across in range(3):
        for along in range(3):
            tap = 3 * (2 - across) + 2 - along
            turned[across, :, along * chans : (along + 1) * chans] = kernel[
                tap * chans : (tap + 1) * chans, :
            ]


def conv_rows(taps, weight, first, rows, turned):
    wide, depth = taps.shape[1], taps.shape[2]
    total = None
    for across in range(3):
        cells = taps[pl.ds(first + across, rows)].reshape(rows * wide, depth)
        dims = (((1,), (1 if turned else 0,)), ((), ()))
        part = lax.dot_general(cells, weight(across), dims, preferred_element_type=F32)
        total = part if total is None else total + part
    return total


def edges_of(array, which, lefts, rights, edge):
    high, wide = array.shape[:2]
    for target, at in ((lefts, 0), (rights, wide - 8)):
        inner = 0 if at == 0 else 7
        for row in range(high):
            strip = array[row, at : at + 8, :].astype(F32)
            edge[row : row + 1, :] = strip[inner : inner + 1, :]
        target[which] = edge[...].astype(BF16)


def identity(cells):
    return cells


def look_kernel(core, upstream, stats, tops, bottoms, lefts, rights, edge):
    high, wide, chans = core.shape

    def step(row, carry):
        cells = core[row].astype(F32)
        return carry[0] + fold(cells), carry[1] + fold(cells * cells)

    zero = jnp.zeros((8, chans), F32)
    stats[...] = pair_rows(*lax.fori_loop(0, high, step, (zero, zero)))
    for which, array in enumerate((core, upstream)):
        tops[which] = array[0]
        bottoms[which] = array[high - 1]
        edges_of(array, which, lefts, rights, edge)


def sides_kernel(flags, lefts, rights, above, below, *refs):
    outs, line = refs[:-1], refs[-1]
    count, high, chans = lefts.shape
    wide = above.shape[1]

    def column(which, edges, at):
        inner = 0 if at == 0 else 7
        line[0:1, :] = above[which, at : at + 8, :].astype(F32)[inner : inner + 1, :]
        line[1 : 1 + high, :] = edges[which].astype(F32)
        line[1 + high : 2 + high, :] = below[which, at : at + 8, :].astype(F32)[
            inner : inner + 1, :
        ]
        return line[...]

    line[...] = jnp.zeros_like(line)
    for which in range(count):
        last = column(which, rights, wide - 8)
        first = column(which, lefts, 0)
        if len(outs) == 1:
            outs[0][which] = jnp.where(flags[3] > 0, last, first).astype(BF16)
        else:
            outs[0][which] = last.astype(BF16)
            outs[1][which] = first.astype(BF16)


def hidden_kernel(
    flags, core, top, bottom, left, right, kernel, stats_a, stats_b, gain, shift,
    hidden, sums, taps, line, sides, *, count,
):
    high, wide, chans = core.shape
    mean, rstd = mean_rstd(stats_a, stats_b, count)
    scale = rstd * gain[...]
    offset = shift[...] - mean * scale
    build_taps(
        flags, core, (top, bottom, left, right), 0, taps, line, sides,
        lambda cells: silu(cells * scale + offset),
    )
    depth = taps.shape[2]

    def step(index, carry):
        block = conv_rows(
            taps,
            lambda across: kernel[across * depth : (across + 1) * depth, :],
            index * CHUNK, CHUNK, False,
        ).astype(BF16)
        hidden[pl.ds(index * CHUNK * wide, CHUNK * wide), :] = block
        wideb = block.astype(F32)
        return carry[0] + fold(wideb), carry[1] + fold(wideb * wideb)

    zero = jnp.zeros((8, chans), F32)
    sums[...] = pair_rows(*lax.fori_loop(0, high // CHUNK, step, (zero, zero)))


def back_conv_kernel(
    flags, core, top, bottom, left, right, kernel, source, stats_a, stats_b, gain, shift,
    out, sums, taps, line, sides, turned, *, count, which,
):
    high, wide, chans = core.shape
    mean, rstd = mean_rstd(stats_a, stats_b, count)
    build_taps(flags, core, (top, bottom, left, right), which, taps, line, sides, identity)
    flip_weights(kernel, turned)

    def step(index, carry):
        window = pl.ds(index * CHUNK * wide, CHUNK * wide)
        grad = conv_rows(taps, lambda across: turned[across], index * CHUNK, CHUNK, True)
        normal = (source[window, :].astype(F32) - mean) * rstd
        block = grad * silu_slope(normal * gain[...] + shift[...])
        out[window, :] = block
        return carry[0] + fold(block), carry[1] + fold(block * normal)

    zero = jnp.zeros((8, chans), F32)
    sums[...] = pair_rows(*lax.fori_loop(0, high // CHUNK, step, (zero, zero)))


def norm_back_terms(stats_a, stats_b, sums_a, sums_b, gain, count):
    mean, rstd = mean_rstd(stats_a, stats_b, count)
    means = group_total((sums_a[...] + sums_b[...]) * gain[...]) / count
    return mean, rstd, means[0:1], means[1:2]


def grad_hidden_kernel(
    grad_pre, hidden, stats_a, stats_b, sums_a, sums_b, gain,
    out, tops, bottoms, lefts, rights, edge, *, count,
):
    mean, rstd, mean_one, mean_two = norm_back_terms(
        stats_a, stats_b, sums_a, sums_b, gain, count
    )
    high, wide, chans = out.shape

    def step(row, carry):
        window = pl.ds(row * wide, wide)
        normal = (hidden[window, :].astype(F32) - mean) * rstd
        block = rstd * (grad_pre[window, :] * gain[...] - mean_one - normal * mean_two)
        out[row] = block.astype(BF16)
        return carry

    lax.fori_loop(0, high, step, 0)
    tops[0] = out[0]
    bottoms[0] = out[high - 1]
    edges_of(out, 0, lefts, rights, edge)


def input_grad_kernel(
    grad_pre, core, upstream, stats_a, stats_b, sums_a, sums_b, gain, out, *, count
):
    mean, rstd, mean_one, mean_two = norm_back_terms(
        stats_a, stats_b, sums_a, sums_b, gain, count
    )
    high, wide, chans = out.shape

    def step(row, carry):
        window = pl.ds(row * wide, wide)
        normal = (core[row].astype(F32) - mean) * rstd
        block = rstd * (grad_pre[window, :] * gain[...] - mean_one - normal * mean_two)
        out[row] = (upstream[row].astype(F32) + block).astype(BF16)
        return carry

    lax.fori_loop(0, high, step, 0)


def scatter_blocks(places, natural, outs, size):
    chans = natural.shape[1]
    whole = chans // LANES
    rest = chans - whole * LANES
    tail = size * rest // LANES
    each = outs[0].shape[0]
    for which, out in enumerate(outs):

        def step(block, carry, which=which, out=out):
            at = pl.multiple_of(places[which * each + block] * size, 8)
            for part in range(whole):
                out[block, part * size : (part + 1) * size, :] = natural[
                    pl.ds(at, size), part * LANES : (part + 1) * LANES
                ]
            for part in range(LANES // rest):
                out[block, whole * size :, part * rest : (part + 1) * rest] = natural[
                    pl.ds(pl.multiple_of(at + part * tail, 8), tail), whole * LANES :
                ]
            return carry

        lax.fori_loop(0, each, step, 0)


def second_grad_kernel(
    flags, places, core, top, bottom, left, right, hidden, stats_a, stats_b, gain, shift,
    keep, send, taps, line, sides, turned, natural, *, count, size,
):
    high, wide, chans = core.shape
    build_taps(flags, core, (top, bottom, left, right), 1, taps, line, sides, identity)
    mean, rstd = mean_rstd(stats_a, stats_b, count)
    scale = rstd * gain[...]
    offset = shift[...] - mean * scale
    depth = taps.shape[2]
    for part in range(high * wide // 256):
        window = slice(part * 256, (part + 1) * 256)
        act = silu(hidden[window, :].astype(F32) * scale + offset)
        turned[:, window] = act.astype(BF16).T
    for across in range(3):
        cells = taps[2 - across : 2 - across + high].reshape(high * wide, depth)
        block = jnp.dot(turned[...], cells, preferred_element_type=F32)
        for along in range(3):
            lanes = slice((2 - along) * chans, (3 - along) * chans)
            first = (3 * across + along) * chans
            natural[first : first + chans, :] = block[:, lanes]
    natural[9 * chans :, :] = jnp.zeros_like(natural[9 * chans :, :])
    scatter_blocks(places, natural, (keep, send), size)


def first_grad_kernel(
    flags, places, core, top, bottom, left, right, grad_hidden, stats_a, stats_b, gain,
    shift, keep, send, taps, line, sides, turned, natural, *, count, size,
):
    high, wide, chans = core.shape
    mean, rstd = mean_rstd(stats_a, stats_b, count)
    scale = rstd * gain[...]
    offset = shift[...] - mean * scale
    build_taps(
        flags, core, (top, bottom, left, right), 0, taps, line, sides,
        lambda cells: silu(cells * scale + offset),
    )
    depth = taps.shape[2]
    rows = 256 // wide
    for part in range(high * wide // 256):
        cells = grad_hidden[part * rows : (part + 1) * rows].reshape(256, chans)
        turned[:, part * 256 : (part + 1) * 256] = cells.T
    for across in range(3):
        cells = taps[across : across + high].reshape(high * wide, depth)
        block = jnp.dot(turned[...], cells, preferred_element_type=F32)
        natural[across * depth : (across + 1) * depth, :] = block.T
    natural[9 * chans :, :] = jnp.zeros_like(natural[9 * chans :, :])
    scatter_blocks(places, natural, (keep, send), size)


def merge_kernel(*refs, terms, layout):
    ins, outs = refs[: -len(layout)], refs[-len(layout) :]
    for out, blocks in zip(outs, layout, strict=True):
        for at, (part, block) in enumerate(blocks):
            total = ins[terms * part][block]
            if terms == 2:
                total = total + ins[2 * part + 1][block]
            out[at] = total.astype(out.dtype)


def spread_kernel(places, mine, other, out, *, size):
    rows, chans = out.shape
    whole = chans // LANES
    rest = chans - whole * LANES
    tail = size * rest // LANES
    each = mine.shape[0]
    for which, source in enumerate((mine, other)):

        def step(block, carry, which=which, source=source):
            place = places[which * each + block]

            @pl.when(place * size < rows)
            def _():
                at = pl.multiple_of(place * size, 8)
                cells = source[block].astype(F32)
                for part in range(whole):
                    out[pl.ds(at, size), part * LANES : (part + 1) * LANES] = cells[
                        part * size : (part + 1) * size
                    ]
                for part in range(LANES // rest):
                    window = pl.ds(pl.multiple_of(at + part * tail, 8), tail)
                    out[window, whole * LANES :] = cells[
                        whole * size :, part * rest : (part + 1) * rest
                    ]

            return carry

        lax.fori_loop(0, each, step, 0)


def swap(value, axis, mask):
    return lax.ppermute(value, axis, [(i, i ^ mask) for i in range(lax.axis_size(axis))])


def bits_of(axis):
    count = lax.axis_size(axis)
    assert count & (count - 1) == 0
    return [(axis, 1 << bit) for bit in range(count.bit_length() - 1)]


def add_up_pair(value, axes):
    *early, (name, mask) = [bit for axis in axes for bit in bits_of(axis)]
    for axis, other in early:
        value = value + swap(value, axis, other)
    return value, swap(value, name, mask)


def shifted(value, axis, step):
    count = lax.axis_size(axis)
    pairs = [(i, i + step) for i in range(count) if 0 <= i + step < count]
    return lax.ppermute(value, axis, pairs)


def borders(flags, tops, bottoms, lefts, rights):
    count, wide, chans = tops.shape
    high = lefts.shape[1]
    above = shifted(bottoms, "row", 1)
    below = shifted(tops, "row", -1)
    pair = lax.axis_size("col") == 2
    out = shape((count, high + 8, chans), BF16)
    sent = call(
        sides_kernel, (out,) if pair else (out, out), 4,
        [pltpu.VMEM((high + 8, chans), F32)], smem=1,
    )(flags, lefts, rights, above, below)
    if pair:
        other = swap(sent[0], "col", 1)
        return above, below, other, other
    return above, below, shifted(sent[0], "col", 1), shifted(sent[1], "col", -1)


def plan():
    row, col, batch = bits_of("row"), bits_of("col"), bits_of("batch")
    return row[:1], row[1:] + col, batch


def exchange_orders():
    first, middle, last = plan()
    return (first + middle + last, first + middle[::-1] + last)


def places_of(blocks):
    half = blocks // 2
    head = len(plan()[0])
    found = []
    for order in exchange_orders():
        own = 0
        for level, (axis, mask) in enumerate(order):
            bit = (lax.axis_index(axis) & mask) // mask
            weight = half >> (level + 1)
            if level < head:
                weight *= 2
            own = own + bit * weight
        found.append(own)
    outer = blocks >> head
    index = jnp.arange(blocks, dtype=jnp.int32)
    chunk = (index % outer) // (outer // 2)
    return index ^ jnp.where(chunk == 0, found[0], found[1])


def merge(parts, layout, dtype=F32):
    terms = len(parts[0])
    tail = parts[0][0].shape[1:]
    return call(
        functools.partial(merge_kernel, terms=terms, layout=layout),
        tuple(shape((len(blocks),) + tail, dtype) for blocks in layout),
        terms * len(parts),
    )(*[array for part in parts for array in part])


def halves(part, first, count):
    blocks = [(part, first + block) for block in range(count)]
    return [blocks[: count // 2], blocks[count // 2 :]]


def give_steps():
    first, middle, last = plan()
    ((axis_one, mask_one),) = first

    def outer(pieces):
        keep, send = pieces
        got = swap(send, axis_one, mask_one)
        count = keep.shape[0]
        layout = halves(0, 0, count // 2) + halves(0, count // 2, count // 2)
        return merge([(keep, got)], layout)

    def chunked(pieces, pair, final):
        got = [swap(pieces[2 * k + 1], axis, mask) for k, (axis, mask) in enumerate(pair)]
        count = pieces[0].shape[0]
        split = [halves(0, 0, count), halves(1, 0, count)]
        layout = split[0] + split[1]
        if final:
            layout = [split[0][k] + split[1][k] for k in range(2)]
        return merge([(pieces[2 * k], got[k]) for k in range(2)], layout)

    def inner(pieces, axis, mask, final):
        got = swap(pieces[1], axis, mask)
        count = pieces[0].shape[0] // 2
        split = [halves(0, 0, count), halves(0, count, count)]
        layout = [split[0][k] + split[1][k] for k in range(2)]
        if final:
            layout = [layout[0] + layout[1]]
        return merge([(pieces[0], got)], layout, BF16 if final else F32)

    steps = [outer]
    pairs = list(zip(middle, middle[::-1], strict=True))
    for level, pair in enumerate(pairs):
        final = level == len(pairs) - 1
        steps.append(functools.partial(chunked, pair=pair, final=final))
    for level, (axis, mask) in enumerate(last):
        final = level == len(last) - 1
        steps.append(functools.partial(inner, axis=axis, mask=mask, final=final))
    return steps


def join(parts, layout):
    return merge([(part,) for part in parts], layout, BF16)


def span(part, count):
    return [(part, block) for block in range(count)]


def take_steps():
    first, middle, last = plan()
    ((axis_one, mask_one),) = first

    def inner(pieces, axis, mask, final):
        (both,) = pieces
        count = both.shape[0]
        blocks = span(0, count) + span(1, count)
        layout = [blocks[0::2], blocks[1::2]] if final else [blocks]
        return join([both, swap(both, axis, mask)], layout)

    def chunked(pieces, pair, final):
        got = [swap(piece, axis, mask) for piece, (axis, mask) in zip(pieces, pair, strict=True)]
        count = pieces[0].shape[0]
        blocks = [span(part, count) for part in range(4)]
        layout = [blocks[0] + blocks[1], blocks[2] + blocks[3]]
        if final:
            layout = [layout[0] + layout[1]]
        return join([pieces[0], got[0], pieces[1], got[1]], layout)

    def outer(pieces):
        return pieces[0], swap(pieces[0], axis_one, mask_one)

    steps = []
    for level, (axis, mask) in enumerate(last[::-1]):
        final = level == len(last) - 1
        steps.append(functools.partial(inner, axis=axis, mask=mask, final=final))
    pairs = list(zip(middle, middle[::-1], strict=True))[::-1]
    for level, pair in enumerate(pairs):
        final = level == len(pairs) - 1
        steps.append(functools.partial(chunked, pair=pair, final=final))
    steps.append(outer)
    return steps


def tie(*values):
    return lax.optimization_barrier(values)


def per_device(
    features, first_kernel, second_kernel, first_gain, first_shift,
    second_gain, second_shift, upstream,
):
    high, wide, chans = features.shape[1:]
    rows, cols = lax.axis_size("row"), lax.axis_size("col")
    devices = rows * cols * lax.axis_size("batch")
    count = float(high * rows * wide * cols * (chans // GROUPS))
    cells = features[0]
    upper = upstream[0]
    weights = [k.reshape(9 * chans, chans) for k in (first_kernel, second_kernel)]
    gains = [g.reshape(1, chans) for g in (first_gain, second_gain)]
    shifts = [s.reshape(1, chans) for s in (first_shift, second_shift)]
    row, col = lax.axis_index("row"), lax.axis_index("col")
    flags = jnp.stack([row > 0, row < rows - 1, col > 0, col < cols - 1]).astype(jnp.int32)
    unit = 2 * devices * 16
    padded = -(-9 * chans // unit) * unit
    blocks = 2 * devices
    size = padded // blocks
    places = places_of(blocks)

    image = shape((high, wide, chans), BF16)
    flat = high * wide
    small = shape((8, chans), F32)
    rows_of = lambda n: shape((n, wide, chans), BF16)
    cols_of = lambda n: shape((n, high, chans), BF16)
    edge = pltpu.VMEM((high, chans), F32)
    tap_scratch = [
        pltpu.VMEM((high + 2, wide, 3 * chans), BF16),
        pltpu.VMEM((wide + 16, chans), F32),
        pltpu.VMEM((2, high + 8, chans), F32),
    ]

    stats_one, *rims = call(
        look_kernel, (small, rows_of(2), rows_of(2), cols_of(2), cols_of(2)), 2, [edge]
    )(cells, upper)
    halo = borders(flags, *rims)
    stats_one = add_up_pair(stats_one, ("row", "col"))
    norm_one = (*stats_one, gains[0], shifts[0])

    hidden, stats_two = call(
        functools.partial(hidden_kernel, count=count),
        (shape((flat, chans), BF16), small), 10, tap_scratch, smem=1,
    )(flags, cells, *halo, weights[0], *norm_one)
    stats_two = add_up_pair(stats_two, ("row", "col"))
    norm_two = (*stats_two, gains[1], shifts[1])

    def back_conv(core, rim, weight, source, norm, which):
        return call(
            functools.partial(back_conv_kernel, count=count, which=which),
            (shape((flat, chans), F32), small), 11,
            tap_scratch + [pltpu.VMEM((3, chans, 3 * chans), BF16)], smem=1,
        )(flags, core, *rim, weight, source, *norm)

    def kernel_grad(body, core, source, norm):
        half = shape((blocks // 2, size * chans // LANES, LANES), F32)
        return call(
            functools.partial(body, count=count, size=size), (half, half), 10,
            tap_scratch + [pltpu.VMEM((chans, flat), BF16), pltpu.VMEM((padded, chans), F32)],
            smem=2,
        )(flags, places, core, *halo, source, *norm)

    give, take = give_steps(), take_steps()
    outward = len(give) - len(plan()[2])
    second = kernel_grad(second_grad_kernel, upper, hidden, norm_two)
    second, norm_two = tie(second, norm_two)

    grad_pre_two, local_two = back_conv(upper, halo, weights[1], hidden, norm_two, 1)
    second, local_two = tie(give[0](second), local_two)
    sums_two = add_up_pair(local_two, ("row", "col"))
    second, sums_two = tie(second, sums_two)

    grad_hidden, *rims = call(
        functools.partial(grad_hidden_kernel, count=count),
        (image, rows_of(1), rows_of(1), cols_of(1), cols_of(1)), 7, [edge],
    )(grad_pre_two, hidden, *norm_two[:2], *sums_two, gains[1])
    rim = borders(flags, *rims)

    first = kernel_grad(first_grad_kernel, cells, grad_hidden, norm_one)
    second = give[1](second)
    second, first, rim, grad_hidden = tie(second, first, rim, grad_hidden)

    grad_pre_one, local_one = back_conv(
        grad_hidden, rim, weights[0], cells.reshape(flat, chans), norm_one, 0
    )
    for step in give[2:outward]:
        second = step(second)
    first, second, local_one = tie(give[0](first), second, local_one)

    small_steps = [(axis, mask) for name in ("row", "col") for axis, mask in bits_of(name)]
    sums_one, other_one = local_one, None
    later = give[outward:] + take
    for level, step in enumerate(give[1:]):
        if level < len(small_steps):
            axis, mask = small_steps[level]
            other_one = swap(sums_one, axis, mask)
            if level < len(small_steps) - 1:
                sums_one = sums_one + other_one
        second = later.pop(0)(second)
        first, second, sums_one, other_one = tie(step(first), second, sums_one, other_one)
    input_grad = call(
        functools.partial(input_grad_kernel, count=count), image, 8
    )(grad_pre_one, cells, upper, *stats_one, sums_one, other_one, gains[0])

    sums = [a + b for a, b in ((sums_one, other_one), sums_two)]
    param = jnp.stack([sums[0][1], sums[0][0], sums[1][1], sums[1][0]])
    batch = bits_of("batch")
    spread = call(
        functools.partial(spread_kernel, size=size), shape((9 * chans, chans), F32), 2, smem=1
    )
    second_grad = None
    for level, step in enumerate(take):
        if level < len(batch):
            axis, mask = batch[level]
            param = param + swap(param, axis, mask)
        if later:
            second = later.pop(0)(second)
        elif second_grad is None:
            second_grad = spread(places, *second)
            first, second_grad = tie(first, second_grad)
        first = step(first)
        if level < len(take) - 1:
            if level == 0:
                first, second, input_grad = tie(first, second, input_grad)
            elif later:
                first, second = tie(first, second)
    if second_grad is None:
        second_grad = spread(places, *second)
    first_grad = spread(places, *first)
    grads = [grad.reshape(3, 3, chans, chans) for grad in (first_grad, second_grad)]
    return (input_grad[None], grads[0], grads[1], param)


def solution(mesh):
    tiled = P("batch", "row", "col", None)
    return jax.shard_map(
        per_device,
        mesh=mesh,
        in_specs=(tiled, P(), P(), P(), P(), P(), P(), tiled),
        out_specs=(tiled, P(), P(), P()),
        check_vma=False,
    )
```
